32 devices in a mesh: gx: 4 (over y, x), gy: 8 (over z, core).
Axes of the slice: x: 2, y: 2, z: 4, core: 2. Of those that a mesh axis runs over, the one named last changes fastest.
Arguments:
- background: float32 [256, 4, 128, 512], P(('gx', 'gy')), may hold values from -6 to 6
- obs_cells: int32 [8, 32, 1024], P('gy', 'gx'), may hold values from 0 to 2303
- obs_counts: int32 [8, 32], P('gy', 'gx'), may hold values from 1 to 1024, as said below
- obs_widths: int32 [8, 32], P('gy', 'gx'), may hold values from 1 to 4
- obs_values: float32 [8, 32, 1024], P('gy', 'gx'), may hold values from -6 to 6
- obs_variances: float32 [8, 32, 1024], P('gy', 'gx'), may hold values from 1 to 16
Outputs:
- analysis: float32 [256, 4, 128, 512], P(('gx', 'gy'))
The draws below stay inside these ranges and needn't reach their ends.
Inputs may be any that keep to these rules, and one draw needn't show every extreme that they name: `obs_cells`: each is level * 24 * 24 + row * 24 + column of a cell in the patch's surrounding region. `obs_counts`: some patch uses all 1024 slots.
All inputs are finite; a program needn't handle non-finite values.
Results may differ from the reference program's by a relative error of at most 0.0003.
Values sent between devices are 32-bit elements; how exact they have to be, the bound alone decides.
A program may use at most 256 MiB of HBM per device.

```python
import math
import jax
import jax.numpy as jnp
from jax import lax

K = 256
LEV = 4
PSIDE = 16
HALO = 4
MAXOBS = 1024
ITERS = 5
PLAT = 8
PLON = 32
NLAT = 128
NLON = 512
AREA = 2304


def draw_obs_counts(key, part):
    latitude = lax.broadcasted_iota(jnp.int32, (PLAT, PLON), 0)
    polar = (latitude * 4 < PLAT) | (latitude * 4 >= 3 * PLAT)
    sparse = jax.random.randint(jax.random.fold_in(key, 11), (PLAT, PLON), 1, MAXOBS // 8 + 1)
    dense = jax.random.randint(jax.random.fold_in(key, 12), (PLAT, PLON), MAXOBS // 4, MAXOBS + 1)
    counts_all = jnp.where(polar, sparse, dense).reshape(-1)
    chosen = jax.random.randint(jax.random.fold_in(key, 13), (), 0, PLAT * PLON)
    counts_all = counts_all.at[chosen].set(MAXOBS)
    return counts_all.reshape(PLAT, PLON).astype(jnp.int32)


def place_ends(result, rng, low, top_value):
    longest = result.shape.index(max(result.shape))
    spots = []
    for shift in (0, 1):
        where = [jax.random.randint(jax.random.fold_in(rng, axis), (), 0, length) for axis, length in enumerate(result.shape)]
        where[longest] = (where[longest] + shift) % result.shape[longest]
        spots.append(tuple(where))
    return result.at[spots[0]].set(low).at[spots[1]].set(top_value)


def steps_of(stream_key, extent, shards, least, high):
    factor_of = 1.0
    for axis_at, shards_of in shards:
        draws = jax.random.uniform(jax.random.fold_in(jax.random.fold_in(stream_key, 6), axis_at), (shards_of,), jnp.float32, least / len(shards), high / len(shards))
        factor_of = factor_of * jnp.repeat(jnp.exp(draws), extent[axis_at] // shards_of).reshape((-1,) + (1,) * (len(extent) - 1 - axis_at))
    return factor_of


def scatter_about(own_key, dims, width, limit, cuts=(), held_as=jnp.bfloat16):
    values = jax.random.normal(own_key, dims, jnp.float32) * width
    if len(cuts) > 0:
        values = steps_of(own_key, dims, cuts, -0.22, 0.18) * values
    return jnp.clip(values, min=-limit, max=limit).astype(held_as)


def setup_inputs(seed: int = 0) -> dict:
    seeds = jax.random.split(jax.random.key(seed), 7)
    background = scatter_about(seeds[0], (K, LEV, NLAT, NLON), 1.0, 6.0, ((0, 32),), jnp.float32)
    obs_cells = place_ends(jax.random.randint(seeds[1], (PLAT, PLON, MAXOBS), 0, AREA), jax.random.fold_in(seeds[1], 1), 0, AREA - 1).astype(jnp.int32)
    obs_counts = draw_obs_counts(jax.random.fold_in(seeds[6], 71), 0)
    obs_widths = place_ends(jax.random.randint(seeds[3], (PLAT, PLON), 1, HALO + 1), jax.random.fold_in(seeds[3], 1), 1, HALO).astype(jnp.int32)
    obs_values = scatter_about(seeds[4], (PLAT, PLON, MAXOBS), 1.0, 6.0, ((0, 8), (1, 4)), jnp.float32)
    obs_variances = jnp.clip(jnp.exp(math.log(16.0) - 2.7725887 * jax.random.uniform(seeds[5], (PLAT, PLON, MAXOBS), jnp.float32) ** steps_of(seeds[5], (PLAT, PLON, MAXOBS), ((0, 8), (1, 4)), -0.2, 0.2)), 1.0, 16.0)
    return dict(background=background, obs_cells=obs_cells, obs_counts=obs_counts, obs_widths=obs_widths, obs_values=obs_values, obs_variances=obs_variances)


def product(former, latter):
    return jnp.einsum('nij,njk->nik', former, latter, precision=lax.Precision.HIGHEST)

def patches_of(region, core_side, margin):
    span_side = core_side + 2 * margin
    amount = (region.shape[3] - 2 * margin) // core_side
    pieces = [region[:, :, :, core_side * patch_index:core_side * patch_index + span_side] for patch_index in range(amount)]
    return jnp.stack(pieces, axis=0)

def observe(patches, obs_cells, obs_counts, obs_widths, obs_values, obs_variances, core_side, margin):
    number = patches.shape[0]
    ensemble_members = patches.shape[1]
    levels = patches.shape[2]
    span_side = patches.shape[3]
    flattened = patches.reshape(number, ensemble_members, levels * span_side * span_side)
    picker = jnp.broadcast_to(obs_cells[:, None, :], (number, ensemble_members, obs_cells.shape[1]))
    sampled = jnp.take_along_axis(flattened, picker, axis=2)
    sampled_mean = lax.optimization_barrier(jnp.mean(sampled, axis=1, keepdims=True))
    observed_spread = sampled - sampled_mean
    innovation = obs_values - sampled_mean[:, 0, :]
    row_pos = obs_cells // span_side % span_side
    col_pos = obs_cells % span_side
    row_out = jnp.maximum(jnp.maximum(margin - row_pos, row_pos - (margin + core_side - 1)), 0)
    col_out = jnp.maximum(jnp.maximum(margin - col_pos, col_pos - (margin + core_side - 1)), 0)
    distance = jnp.maximum(row_out, col_out)
    slot_ids = lax.broadcasted_iota(jnp.int32, obs_cells.shape, 1)
    usable = (slot_ids < obs_counts[:, None]) & (distance <= obs_widths[:, None])
    relative = distance.astype(jnp.float32) / (obs_widths[:, None] + 1).astype(jnp.float32)
    weights = jnp.where(usable, jnp.exp(-relative * relative) / obs_variances, 0.0)
    scaled_spread = observed_spread * weights[:, None, :]
    pulled = lax.optimization_barrier(jnp.sum(scaled_spread * innovation[:, None, :], axis=2))
    return (scaled_spread, observed_spread, pulled)

def settle(gram_sum, pulled, patches, core_side, margin, sweeps):
    ensemble_members = gram_sum.shape[1]
    identity_m = jnp.eye(ensemble_members, dtype=jnp.float32)
    frobenius = jnp.sqrt(lax.optimization_barrier(jnp.sum(gram_sum * gram_sum, axis=(1, 2))))
    divisor = ensemble_members - 1.0 + frobenius
    current = (gram_sum + (ensemble_members - 1.0) * identity_m) / divisor[:, None, None]
    inverse_root = jnp.broadcast_to(identity_m, gram_sum.shape)
    for repeat in range(sweeps):
        factor = 1.5 * identity_m - 0.5 * product(inverse_root, current)
        current = product(current, factor)
        inverse_root = product(factor, inverse_root)
    halfway = jnp.einsum('nkj,nj->nk', inverse_root, pulled, precision=lax.Precision.HIGHEST)
    mean_weight = jnp.einsum('nkj,nj->nk', inverse_root, halfway, precision=lax.Precision.HIGHEST) / divisor[:, None]
    combined = jnp.sqrt((ensemble_members - 1.0) / divisor)[:, None, None] * inverse_root + mean_weight[:, :, None]
    core_cells = patches[:, :, :, margin:margin + core_side, margin:margin + core_side]
    patch_centre = lax.optimization_barrier(jnp.mean(core_cells, axis=1, keepdims=True))
    deviation = core_cells - patch_centre
    return patch_centre + jnp.einsum('njk,njlab->nklab', combined, deviation, precision=lax.Precision.HIGHEST)

def assemble(analysed):
    number = analysed.shape[0]
    ensemble_members = analysed.shape[1]
    levels = analysed.shape[2]
    core_side = analysed.shape[3]
    moved = jnp.transpose(analysed, (1, 2, 3, 0, 4))
    return moved.reshape(ensemble_members, levels, core_side, number * core_side)

def reference(background, obs_cells, obs_counts, obs_widths, obs_values, obs_variances):
    padded_state = jnp.pad(background, ((0, 0), (0, 0), (HALO, HALO), (0, 0)))
    padded_state = jnp.concatenate([padded_state[:, :, :, -HALO:], padded_state, padded_state[:, :, :, :HALO]], axis=3)

    def one_band(packed_state):
        band_index, band_cells, band_counts, band_widths, band_values, band_variances = packed_state
        region = lax.dynamic_slice_in_dim(padded_state, band_index * PSIDE, PSIDE + 2 * HALO, 2)
        patches = patches_of(region, PSIDE, HALO)
        scaled_spread, observed_spread, pulled = observe(patches, band_cells, band_counts, band_widths, band_values, band_variances, PSIDE, HALO)
        gram_sum = jnp.einsum('nkm,njm->nkj', scaled_spread, observed_spread, precision=lax.Precision.HIGHEST)
        return assemble(settle(gram_sum, pulled, patches, PSIDE, HALO, ITERS))
    bands = lax.map(one_band, (jnp.arange(PLAT, dtype=jnp.int32), obs_cells, obs_counts, obs_widths, obs_values, obs_variances))
    return jnp.transpose(bands, (1, 2, 0, 3, 4)).reshape(K, LEV, NLAT, NLON)
```

```python
import functools

import jax
import jax.numpy as jnp
from jax import lax
from jax.experimental import pallas as pl
from jax.experimental.pallas import tpu as pltpu
from jax.sharding import PartitionSpec as P

PSIDE = 16
HALO = 4
ITERS = 5
SUB = 8
SPAN = PSIDE + 2 * HALO
HIGHEST = lax.Precision.HIGHEST
VMEM_LIMIT = 48 * 1024 * 1024


def split(x):
    high = x.astype(jnp.bfloat16)
    return high, (x - high.astype(jnp.float32)).astype(jnp.bfloat16)


def dot3(a, b, dims=((1,), (0,))):
    def one(x, y):
        return lax.dot_general(x, y, (dims, ((), ())), preferred_element_type=jnp.float32)

    return one(a[0], b[0]) + (one(a[0], b[1]) + one(a[1], b[0]))


def gram_kernel(first, unroll, core, up, down, left, right, tables, *rest):
    if first:
        gram, pulled, band = rest
    else:
        gram_in, pulled_in, gram, pulled, band = rest
    number = tables.shape[0]
    members = core.shape[2]
    lon = core.shape[1]
    rows = core.shape[0]
    band[0:HALO, SUB : SUB + lon] = up[...]
    band[HALO : HALO + rows, SUB : SUB + lon] = core[...]
    band[HALO + rows : SPAN, SUB : SUB + lon] = down[...]
    band[:, 0:SUB] = left[...]
    band[:, SUB + lon :] = right[...]
    cells = SPAN * SUB
    cell_row = lax.broadcasted_iota(jnp.int32, (cells, SPAN), 0) // SUB
    expand = (cell_row == lax.broadcasted_iota(jnp.int32, (cells, SPAN), 1)).astype(jnp.float32)
    sub = lax.broadcasted_iota(jnp.int32, (cells, 2 * SPAN), 0) % SUB
    lane = lax.broadcasted_iota(jnp.int32, (cells, 2 * SPAN), 1)
    near = lax.broadcasted_iota(jnp.int32, (SPAN, SUB, members), 1) < HALO

    def step(block, carry):
        for inner in range(unroll):
            p = block * unroll + inner
            base = pl.multiple_of(p * PSIDE, SUB)

            def columns(k):
                return band[:, pl.ds(pl.multiple_of(base + k * SUB, SUB), SUB), :]

            pieces = [columns(1), columns(2), jnp.where(near, columns(3), columns(0))]
            table = jnp.dot(
                expand, tables[p], precision=HIGHEST, preferred_element_type=jnp.float32
            )
            spread, scaled, pull = [], [], 0.0
            for g, piece in enumerate(pieces):
                x = piece.reshape(cells, members)
                mean = jnp.mean(x, axis=1, keepdims=True)
                y = x - mean
                w = jnp.sum(jnp.where(lane == g * SUB + sub, table, 0.0), axis=1, keepdims=True)
                u = jnp.sum(
                    jnp.where(lane == SPAN + g * SUB + sub, table, 0.0), axis=1, keepdims=True
                )
                pull = pull + jnp.sum(y * (u - w * mean), axis=0, keepdims=True)
                spread.append(y)
                scaled.append(y * w)
            y = split(jnp.concatenate(spread, axis=0))
            z = split(jnp.concatenate(scaled, axis=0))
            total = dot3(z, y, ((0,), (0,)))
            if first:
                gram[p] = total
                pulled[p] = pull
            else:
                gram[p] = gram_in[p] + total
                pulled[p] = pulled_in[p] + pull
        return carry

    lax.fori_loop(0, number // unroll, step, 0)


def root_kernel(unroll, sweeps, gram, pulled, high_ref, low_ref, mean_ref):
    number = gram.shape[0]
    members = gram.shape[1]
    eye = (
        lax.broadcasted_iota(jnp.int32, (members, members), 0)
        == lax.broadcasted_iota(jnp.int32, (members, members), 1)
    ).astype(jnp.float32)

    def step(block, carry):
        ids = [block * unroll + inner for inner in range(unroll)]
        divisors, currents = [], []
        for p in ids:
            g = gram[p]
            square = jnp.sum(jnp.sum(g * g, axis=0, keepdims=True), axis=1, keepdims=True)
            divisor = members - 1.0 + jnp.sqrt(square)
            divisors.append(divisor)
            currents.append((g + (members - 1.0) * eye) / divisor)
        roots = None
        for repeat in range(sweeps):
            cur = [split(c) for c in currents]
            if repeat == 0:
                factors = [1.5 * eye - 0.5 * c for c in currents]
                fac = [split(f) for f in factors]
                roots = factors
            else:
                old = [split(r) for r in roots]
                factors = [1.5 * eye - 0.5 * dot3(r, c) for r, c in zip(old, cur)]
                fac = [split(f) for f in factors]
                roots = [dot3(f, r) for f, r in zip(fac, old)]
            if repeat < sweeps - 1:
                currents = [dot3(c, f) for c, f in zip(cur, fac)]
        for p, divisor, root in zip(ids, divisors, roots):
            half = jnp.sum(root * pulled[p], axis=1, keepdims=True)
            mean_ref[p] = jnp.sum(root * half, axis=0, keepdims=True) / divisor
            high, low = split(jnp.sqrt((members - 1.0) / divisor) * root)
            high_ref[p] = high
            low_ref[p] = low
        return carry

    lax.fori_loop(0, number // unroll, step, 0)


def apply_kernel(unroll, core, high_ref, low_ref, mean_ref, out):
    number = high_ref.shape[0]
    rows = core.shape[0]
    members = core.shape[2]

    def step(block, carry):
        for inner in range(unroll):
            p = block * unroll + inner
            where = pl.ds(pl.multiple_of(p * PSIDE, PSIDE), PSIDE)
            x = core[:, where, :].reshape(rows * PSIDE, members)
            centre = jnp.mean(x, axis=1, keepdims=True)
            d = x - centre
            shift = centre + jnp.sum(d * mean_ref[p], axis=1, keepdims=True)
            mixed = shift + dot3(split(d), (high_ref[p], low_ref[p]))
            out[:, where, :] = mixed.reshape(rows, PSIDE, members)
        return carry

    lax.fori_loop(0, number // unroll, step, 0)


def vmem(count):
    return [pl.BlockSpec(memory_space=pltpu.VMEM)] * count


def call(kernel, outs, inputs, flops, scratch=(), aliases=None):
    moved = sum(a.size * a.dtype.itemsize for a in (*inputs, *outs))
    return pl.pallas_call(
        kernel,
        out_shape=outs,
        in_specs=vmem(len(inputs)),
        out_specs=vmem(len(outs)),
        scratch_shapes=list(scratch),
        input_output_aliases=aliases or {},
        compiler_params=pltpu.CompilerParams(vmem_limit_bytes=VMEM_LIMIT),
        cost_estimate=pl.CostEstimate(flops=flops, bytes_accessed=moved, transcendentals=0),
    )(*inputs)


def tables_of(obs_cells, obs_counts, obs_widths, obs_values, obs_variances, levels):
    level_of = obs_cells // (SPAN * SPAN)
    row = obs_cells // SPAN % SPAN
    col = obs_cells % SPAN
    row_out = jnp.maximum(jnp.maximum(HALO - row, row - (HALO + PSIDE - 1)), 0)
    col_out = jnp.maximum(jnp.maximum(HALO - col, col - (HALO + PSIDE - 1)), 0)
    distance = jnp.maximum(row_out, col_out)
    slots = lax.broadcasted_iota(jnp.int32, obs_cells.shape, 1)
    usable = (slots < obs_counts[:, None]) & (distance <= obs_widths[:, None])
    relative = distance.astype(jnp.float32) / (obs_widths[:, None] + 1).astype(jnp.float32)
    weights = jnp.where(usable, jnp.exp(-relative * relative) / obs_variances, 0.0)
    place = jnp.where(
        col < HALO,
        PSIDE + HALO + col,
        col - HALO,
    )
    line = level_of * SPAN + row
    hot_line = (line[:, :, None] == jnp.arange(levels * SPAN)).astype(jnp.float32)
    hot_place = place[:, :, None] == jnp.arange(SPAN)
    sums = jnp.concatenate(
        [
            jnp.where(hot_place, weights[:, :, None], 0.0),
            jnp.where(hot_place, (weights * obs_values)[:, :, None], 0.0),
        ],
        axis=2,
    )
    table = jnp.einsum("psl,psg->plg", hot_line, sums, precision=HIGHEST)
    return table.reshape(table.shape[0], levels, SPAN, 2 * SPAN)


def shift(x, axis, step, wrap):
    n = lax.axis_size(axis)
    pairs = [(i, (i + step) % n) for i in range(n) if wrap or 0 <= i + step < n]
    return lax.ppermute(x, axis, pairs)


def shards(background, obs_cells, obs_counts, obs_widths, obs_values, obs_variances):
    here, levels, lat_rows, lon_cells = background.shape
    nx = lax.axis_size("gx")
    ny = lax.axis_size("gy")
    lat = lat_rows // ny
    lon = lon_cells // nx
    members = nx * ny * here
    number = lon // PSIDE
    tables = tables_of(
        obs_cells[0], obs_counts[0], obs_widths[0], obs_values[0], obs_variances[0], levels
    )
    cores, state = [], ()
    for level in range(levels):
        arranged = background[:, level].reshape(here, ny, lat, nx, lon)
        arranged = jnp.transpose(arranged, (3, 1, 0, 2, 4)).reshape(members, lat, lon)
        gathered = lax.all_to_all(arranged, ("gx", "gy"), split_axis=0, concat_axis=0, tiled=True)
        core = jnp.transpose(gathered, (1, 2, 0))
        cores.append(core)
        up = shift(core[lat - HALO :], "gy", 1, False)
        down = shift(core[:HALO], "gy", -1, False)

        def edge(side):
            return jnp.concatenate([up[:, side], core[:, side], down[:, side]], axis=0)

        left = shift(edge(slice(lon - SUB, lon)), "gx", 1, True)
        right = shift(edge(slice(0, SUB)), "gx", -1, True)
        inputs = (core, up, down, left, right, tables[:, level], *state)
        state = call(
            functools.partial(gram_kernel, level == 0, 2),
            (
                jax.ShapeDtypeStruct((number, members, members), jnp.float32),
                jax.ShapeDtypeStruct((number, 1, members), jnp.float32),
            ),
            inputs,
            6 * number * members * members * SPAN * SPAN,
            scratch=[pltpu.VMEM((SPAN, lon + 2 * SUB, members), jnp.float32)],
            aliases=None if level == 0 else {6: 0, 7: 1},
        )
    square = jax.ShapeDtypeStruct((number, members, members), jnp.bfloat16)
    transform = call(
        functools.partial(root_kernel, 2, ITERS),
        (square, square, jax.ShapeDtypeStruct((number, 1, members), jnp.float32)),
        state,
        72 * number * members**3,
    )
    results = []
    for level in range(levels):
        (mixed,) = call(
            functools.partial(apply_kernel, 2),
            (jax.ShapeDtypeStruct((lat, lon, members), jnp.float32),),
            (cores[level], *transform),
            6 * lat * lon * members * members,
        )
        mixed = jnp.transpose(mixed, (2, 0, 1))
        returned = lax.all_to_all(mixed, ("gx", "gy"), split_axis=0, concat_axis=0, tiled=True)
        returned = returned.reshape(nx, ny, here, lat, lon)
        results.append(jnp.transpose(returned, (2, 1, 3, 0, 4)).reshape(here, lat_rows, lon_cells))
    return jnp.stack(results, axis=1)


def solution(mesh):
    return jax.shard_map(
        shards,
        mesh=mesh,
        in_specs=(
            P(("gx", "gy"), None, None, None),
            P("gy", "gx", None),
            P("gy", "gx"),
            P("gy", "gx"),
            P("gy", "gx", None),
            P("gy", "gx", None),
        ),
        out_specs=P(("gx", "gy"), None, None, None),
        check_vma=False,
    )
```

```python
import functools

import jax
import jax.numpy as jnp
from jax import lax
from jax.experimental import pallas as pl
from jax.experimental.pallas import tpu as pltpu
from jax.sharding import PartitionSpec as P

PSIDE = 16
HALO = 4
ITERS = 5
SUB = 8
SPAN = PSIDE + 2 * HALO
HIGHEST = lax.Precision.HIGHEST
VMEM_LIMIT = 32 * 1024 * 1024
SMALL_LIMIT = 60 * 1024 * 1024


def split(x):
    high = x.astype(jnp.bfloat16)
    return high, (x - high.astype(jnp.float32)).astype(jnp.bfloat16)


def dot3(a, b, dims=((1,), (0,))):
    def one(x, y):
        return lax.dot_general(x, y, (dims, ((), ())), preferred_element_type=jnp.float32)

    return one(a[0], b[0]) + (one(a[0], b[1]) + one(a[1], b[0]))


def pack_kernel(ny, offset, width, source, out):
    levels = source.shape[1]
    lat = source.shape[2] // ny
    lon = source.shape[3] // out.shape[0]
    for x in range(out.shape[0]):
        begin = x * lon + offset
        parts = [source[0, level, :, begin : begin + width] for level in range(levels)]
        out[x, :, 0] = jnp.concatenate(parts, axis=1).reshape(ny, lat, levels * width)


def unpack_kernel(ny, *refs):
    *chunks, out = refs
    levels = out.shape[1]
    for x in range(chunks[0].shape[0]):
        for level in range(levels):
            begin = level * 2 * PSIDE
            parts = [chunks[-1][x, :, 0, :, begin + PSIDE : begin + 2 * PSIDE]]
            parts += [chunk[x, :, 0, :, begin : begin + 2 * PSIDE] for chunk in chunks[:-1]]
            parts += [chunks[-1][x, :, 0, :, begin : begin + PSIDE]]
            whole = jnp.concatenate(parts, axis=2)
            lon = whole.shape[2]
            out[0, level, :, x * lon : (x + 1) * lon] = whole.reshape(-1, lon)


def roots_of(grams, pulls, sweeps):
    members = grams[0].shape[0]
    eye = (
        lax.broadcasted_iota(jnp.int32, (members, members), 0)
        == lax.broadcasted_iota(jnp.int32, (members, members), 1)
    ).astype(jnp.float32)
    divisors, currents = [], []
    for g in grams:
        square = jnp.sum(jnp.sum(g * g, axis=0, keepdims=True), axis=1, keepdims=True)
        divisor = members - 1.0 + jnp.sqrt(square)
        divisors.append(divisor)
        currents.append((g + (members - 1.0) * eye) / divisor)
    roots = None
    for repeat in range(sweeps):
        cur = [split(c) for c in currents]
        if repeat == 0:
            factors = [1.5 * eye - 0.5 * c for c in currents]
            fac = [split(f) for f in factors]
            roots = factors
        else:
            old = [split(r) for r in roots]
            factors = [1.5 * eye - 0.5 * dot3(r, c) for r, c in zip(old, cur)]
            fac = [split(f) for f in factors]
            roots = [dot3(f, r) for f, r in zip(fac, old)]
        if repeat < sweeps - 1:
            currents = [dot3(c, f) for c, f in zip(cur, fac)]
    results = []
    for divisor, root, pull in zip(divisors, roots, pulls):
        half = jnp.sum(root * pull, axis=1, keepdims=True)
        mean = jnp.sum(root * half, axis=0, keepdims=True) / divisor
        results.append((split(jnp.sqrt((members - 1.0) / divisor) * root), mean))
    return results


def pair_kernel(inside, *refs):
    first, second, refs = refs[:3], refs[3:6], refs[6:]
    if inside:
        tables, out, gram, pulled = refs
    else:
        after, before, tables, out, gram, pulled = refs
    rows, lanes, members = first[1].shape
    levels = tables.shape[1]
    width = lanes // levels
    cells = SPAN * SUB
    cell_row = lax.broadcasted_iota(jnp.int32, (cells, SPAN), 0) // SUB
    expand = (cell_row == lax.broadcasted_iota(jnp.int32, (cells, SPAN), 1)).astype(jnp.float32)
    sub = lax.broadcasted_iota(jnp.int32, (cells, 2 * SPAN), 0) % SUB
    lane = lax.broadcasted_iota(jnp.int32, (cells, 2 * SPAN), 1)
    near = lax.broadcasted_iota(jnp.int32, (SPAN, SUB, members), 1) < HALO
    gram[...] = jnp.zeros_like(gram)
    pulled[...] = jnp.zeros_like(pulled)

    def step(level, carry):
        def block(group, offset):
            where = pl.ds(pl.multiple_of(level * width + offset, SUB), SUB)
            return jnp.concatenate([ref[:, where, :] for ref in group], axis=0)

        def outside(ref):
            return ref[:, pl.ds(pl.multiple_of(level * SUB, SUB), SUB), :]

        right = block(second, 0) if inside else outside(after)
        left = block(first, width - SUB) if inside else outside(before)
        both = [
            (
                block(first, PSIDE),
                block(first, PSIDE + SUB),
                jnp.where(near, right, block(first, PSIDE - SUB)),
            ),
            (block(second, 0), block(second, SUB), jnp.where(near, block(second, PSIDE), left)),
        ]
        for p, pieces in enumerate(both):
            table = jnp.dot(
                expand, tables[p, level], precision=HIGHEST, preferred_element_type=jnp.float32
            )
            spread, scaled, pull = [], [], 0.0
            for g, piece in enumerate(pieces):
                x = piece.reshape(cells, members)
                mean = jnp.mean(x, axis=1, keepdims=True)
                y = x - mean
                w = jnp.sum(jnp.where(lane == g * SUB + sub, table, 0.0), axis=1, keepdims=True)
                u = jnp.sum(
                    jnp.where(lane == SPAN + g * SUB + sub, table, 0.0), axis=1, keepdims=True
                )
                pull = pull + jnp.sum(y * (u - w * mean), axis=0, keepdims=True)
                spread.append(y)
                scaled.append(y * w)
            y = split(jnp.concatenate(spread, axis=0))
            z = split(jnp.concatenate(scaled, axis=0))
            gram[p] += dot3(z, y, ((0,), (0,)))
            pulled[p] += pull
        return carry

    lax.fori_loop(0, levels, step, 0)
    results = roots_of([gram[0], gram[1]], [pulled[0], pulled[1]], ITERS)
    for p, (group, offset) in enumerate(((first, PSIDE), (second, 0))):
        root, mean_weight = results[p]
        for level in range(levels):
            x = group[1][:, level * width + offset : level * width + offset + PSIDE, :]
            x = x.reshape(rows * PSIDE, members)
            centre = jnp.mean(x, axis=1, keepdims=True)
            d = x - centre
            moved = centre + jnp.sum(d * mean_weight, axis=1, keepdims=True)
            mixed = moved + dot3(split(d), root)
            begin = level * width + p * PSIDE
            out[:, begin : begin + PSIDE, :] = mixed.reshape(rows, PSIDE, members)


def estimate(flops, *arrays):
    moved = sum(a.size * a.dtype.itemsize for a in arrays)
    return pl.CostEstimate(flops=flops, bytes_accessed=moved, transcendentals=0)


def pack(background, nx, ny, offset, width):
    here, levels, lat_rows, lon_cells = background.shape
    lat = lat_rows // ny
    shape = jax.ShapeDtypeStruct((nx, ny, here, lat, levels * width), background.dtype)
    return pl.pallas_call(
        functools.partial(pack_kernel, ny, offset, width),
        out_shape=shape,
        grid=(here,),
        in_specs=[pl.BlockSpec((1, levels, lat_rows, lon_cells), lambda h: (h, 0, 0, 0))],
        out_specs=pl.BlockSpec((nx, ny, 1, lat, levels * width), lambda h: (0, 0, h, 0, 0)),
        cost_estimate=estimate(0, background, shape),
        compiler_params=pltpu.CompilerParams(vmem_limit_bytes=SMALL_LIMIT),
    )(background)


def unpack(chunks, shape):
    nx, ny, here, lat, lanes = chunks[0].shape
    return pl.pallas_call(
        functools.partial(unpack_kernel, ny),
        out_shape=jax.ShapeDtypeStruct(shape, chunks[0].dtype),
        grid=(here,),
        in_specs=[pl.BlockSpec((nx, ny, 1, lat, lanes), lambda h: (0, 0, h, 0, 0))] * len(chunks),
        out_specs=pl.BlockSpec((1, *shape[1:]), lambda h: (h, 0, 0, 0)),
        cost_estimate=estimate(0, *chunks, *chunks),
        compiler_params=pltpu.CompilerParams(vmem_limit_bytes=SMALL_LIMIT),
    )(*chunks)


def analyse(inside, inputs, levels):
    core = inputs[1]
    members = core.shape[2]
    shape = jax.ShapeDtypeStruct(core.shape, core.dtype)
    vmem = pl.BlockSpec(memory_space=pltpu.VMEM)
    flops = 6 * 2 * members**2 * (levels * SPAN * SPAN + levels * PSIDE * PSIDE + 12 * members)
    return pl.pallas_call(
        functools.partial(pair_kernel, inside),
        out_shape=shape,
        in_specs=[vmem] * len(inputs),
        out_specs=vmem,
        scratch_shapes=[
            pltpu.VMEM((2, members, members), jnp.float32),
            pltpu.VMEM((2, 1, members), jnp.float32),
        ],
        cost_estimate=estimate(5 * flops, *inputs, shape),
        compiler_params=pltpu.CompilerParams(vmem_limit_bytes=VMEM_LIMIT),
    )(*inputs)


def tables_of(obs_cells, obs_counts, obs_widths, obs_values, obs_variances, levels):
    level_of = obs_cells // (SPAN * SPAN)
    row = obs_cells // SPAN % SPAN
    col = obs_cells % SPAN
    row_out = jnp.maximum(jnp.maximum(HALO - row, row - (HALO + PSIDE - 1)), 0)
    col_out = jnp.maximum(jnp.maximum(HALO - col, col - (HALO + PSIDE - 1)), 0)
    distance = jnp.maximum(row_out, col_out)
    slots = lax.broadcasted_iota(jnp.int32, obs_cells.shape, 1)
    usable = (slots < obs_counts[:, None]) & (distance <= obs_widths[:, None])
    relative = distance.astype(jnp.float32) / (obs_widths[:, None] + 1).astype(jnp.float32)
    weights = jnp.where(usable, jnp.exp(-relative * relative) / obs_variances, 0.0)
    place = jnp.where(
        col < HALO,
        PSIDE + HALO + col,
        col - HALO,
    )
    line = level_of * SPAN + row
    hot_line = (line[:, :, None] == jnp.arange(levels * SPAN)).astype(jnp.float32)
    hot_place = place[:, :, None] == jnp.arange(SPAN)
    sums = jnp.concatenate(
        [
            jnp.where(hot_place, weights[:, :, None], 0.0),
            jnp.where(hot_place, (weights * obs_values)[:, :, None], 0.0),
        ],
        axis=2,
    )
    table = jnp.einsum("psl,psg->plg", hot_line, sums, precision=HIGHEST)
    return table.reshape(table.shape[0], levels, SPAN, 2 * SPAN)


def shift(x, axis, step, wrap):
    n = lax.axis_size(axis)
    pairs = [(i, (i + step) % n) for i in range(n) if wrap or 0 <= i + step < n]
    return lax.ppermute(x, axis, pairs)


def shards(background, obs_cells, obs_counts, obs_widths, obs_values, obs_variances):
    here, levels, lat_rows, lon_cells = background.shape
    nx = lax.axis_size("gx")
    ny = lax.axis_size("gy")
    lat = lat_rows // ny
    lon = lon_cells // nx
    members = nx * ny * here
    width = 2 * PSIDE
    number = lon // width
    tables = tables_of(
        obs_cells[0], obs_counts[0], obs_widths[0], obs_values[0], obs_variances[0], levels
    )

    def exchange(x):
        return lax.all_to_all(x, ("gx", "gy"), split_axis=0, concat_axis=0, tiled=True)

    def section(group, begin):
        def pick(x):
            x = x.reshape(x.shape[0], levels, width, members)[:, :, begin : begin + SUB]
            return x.reshape(x.shape[0], levels * SUB, members)

        return jnp.concatenate([pick(x) for x in group], axis=0)

    packed = [
        pack(background, nx, ny, q * width, width).reshape(members, lat, levels * width)
        for q in range(number)
    ]
    groups, mixed = [], []
    for q in range(number):
        send = packed[q]
        if q >= 3:
            send, mixed[q - 3] = lax.optimization_barrier((send, mixed[q - 3]))
        gathered = exchange(send)
        core = jnp.transpose(gathered, (1, 2, 0))
        up = shift(core[lat - HALO :], "gy", 1, False)
        down = shift(core[:HALO], "gy", -1, False)
        groups.append((up, core, down))
        if q == 0:
            after = shift(section(groups[0], 0), "gx", -1, True)
        if q in range(1, number - 1):
            table = tables[2 * q - 1 : 2 * q + 1]
            mixed.append(analyse(True, (*groups[q - 1], *groups[q], table), levels))
    q = number - 1
    mixed[0], gathered, mixed[-1] = lax.optimization_barrier((mixed[0], gathered, mixed[-1]))
    before = shift(section(groups[-1], width - SUB), "gx", 1, True)
    table = tables[2 * q - 1 : 2 * q + 1]
    mixed.append(analyse(True, (*groups[q - 1], *groups[q], table), levels))
    table = jnp.stack([tables[-1], tables[0]])
    mixed.append(analyse(False, (*groups[-1], *groups[0], after, before, table), levels))
    chunks = []
    for c in range(number):
        back = jnp.transpose(mixed[c], (2, 0, 1))
        if 0 < c < number - 1:
            back, mixed[c + 1] = lax.optimization_barrier((back, mixed[c + 1]))
        chunks.append(exchange(back).reshape(nx, ny, here, lat, levels * width))
    return unpack(chunks, background.shape)


def solution(mesh):
    return jax.shard_map(
        shards,
        mesh=mesh,
        in_specs=(
            P(("gx", "gy"), None, None, None),
            P("gy", "gx", None),
            P("gy", "gx"),
            P("gy", "gx"),
            P("gy", "gx", None),
            P("gy", "gx", None),
        ),
        out_specs=P(("gx", "gy"), None, None, None),
        check_vma=False,
    )
```

```python
import functools

import jax
import jax.numpy as jnp
from jax import lax
from jax.experimental import pallas as pl
from jax.experimental.pallas import tpu as pltpu
from jax.sharding import PartitionSpec as P

PSIDE = 16
HALO = 4
ITERS = 5
SUB = 8
SPAN = PSIDE + 2 * HALO
HIGHEST = lax.Precision.HIGHEST
VMEM_LIMIT = 32 * 1024 * 1024
SMALL_LIMIT = 60 * 1024 * 1024


def split(x):
    high = x.astype(jnp.bfloat16)
    return high, (x - high.astype(jnp.float32)).astype(jnp.bfloat16)


def dot3(a, b, dims=((1,), (0,))):
    def one(x, y):
        return lax.dot_general(x, y, (dims, ((), ())), preferred_element_type=jnp.float32)

    return one(a[0], b[0]) + (one(a[0], b[1]) + one(a[1], b[0]))


def pack_kernel(ny, turn, width, source, out):
    levels = source.shape[1]
    lat = source.shape[2] // ny
    lon = source.shape[3] // out.shape[0]
    shape = (source.shape[2], lon)
    group = lax.broadcasted_iota(jnp.int32, shape, 1) // width
    for x in range(out.shape[0]):
        whole = source[0, 0, :, x * lon : (x + 1) * lon]
        for level in range(1, levels):
            part = source[0, level, :, x * lon : (x + 1) * lon]
            part = pltpu.roll(part, level * width, 1)
            whole = jnp.where(group == (turn + level) % levels, part, whole)
        out[x, :, 0] = whole.reshape(ny, lat, lon)


def unpack_kernel(*refs):
    *chunks, out = refs
    levels = out.shape[1]
    ny, lat, lon = chunks[0].shape[1], chunks[0].shape[3], chunks[0].shape[4]
    width = lon // levels
    group = lax.broadcasted_iota(jnp.int32, (ny * lat, lon), 1) // width
    for x in range(chunks[0].shape[0]):
        parts = [chunk[x, :, 0].reshape(ny * lat, lon) for chunk in chunks]
        for level in range(levels):
            whole = parts[0]
            for turn in range(1, len(parts)):
                whole = jnp.where(group == (turn + level) % levels, parts[turn], whole)
            back = (PSIDE - level * width) % lon
            out[0, level, :, x * lon : (x + 1) * lon] = pltpu.roll(whole, back, 1)


def roots_of(grams, pulls, sweeps):
    members = grams[0].shape[0]
    eye = (
        lax.broadcasted_iota(jnp.int32, (members, members), 0)
        == lax.broadcasted_iota(jnp.int32, (members, members), 1)
    ).astype(jnp.float32)
    divisors, currents = [], []
    for g in grams:
        square = jnp.sum(jnp.sum(g * g, axis=0, keepdims=True), axis=1, keepdims=True)
        divisor = members - 1.0 + jnp.sqrt(square)
        divisors.append(divisor)
        currents.append((g + (members - 1.0) * eye) / divisor)
    roots = None
    for repeat in range(sweeps):
        cur = [split(c) for c in currents]
        if repeat == 0:
            factors = [1.5 * eye - 0.5 * c for c in currents]
            fac = [split(f) for f in factors]
            roots = factors
        else:
            old = [split(r) for r in roots]
            factors = [1.5 * eye - 0.5 * dot3(r, c) for r, c in zip(old, cur)]
            fac = [split(f) for f in factors]
            roots = [dot3(f, r) for f, r in zip(fac, old)]
        if repeat < sweeps - 1:
            currents = [dot3(c, f) for c, f in zip(cur, fac)]
    results = []
    for divisor, root, pull in zip(divisors, roots, pulls):
        half = jnp.sum(root * pull, axis=1, keepdims=True)
        mean = jnp.sum(root * half, axis=0, keepdims=True) / divisor
        results.append((split(jnp.sqrt((members - 1.0) / divisor) * root), mean))
    return results


def pair_kernel(turn, inside, *refs):
    first, second, refs = (refs[:3], turn), (refs[3:6], turn + 1), refs[6:]
    if inside:
        tables, _, out, gram, pulled = refs
    else:
        after, before, tables, _, out, gram, pulled = refs
    rows, lanes, members = first[0][1].shape
    levels = tables.shape[1]
    width = lanes // levels
    cells = SPAN * SUB
    cell_row = lax.broadcasted_iota(jnp.int32, (cells, SPAN), 0) // SUB
    expand = (cell_row == lax.broadcasted_iota(jnp.int32, (cells, SPAN), 1)).astype(jnp.float32)
    sub = lax.broadcasted_iota(jnp.int32, (cells, 2 * SPAN), 0) % SUB
    lane = lax.broadcasted_iota(jnp.int32, (cells, 2 * SPAN), 1)
    near = lax.broadcasted_iota(jnp.int32, (SPAN, SUB, members), 1) < HALO
    gram[...] = jnp.zeros_like(gram)
    pulled[...] = jnp.zeros_like(pulled)

    def step(level, carry):
        def block(group, offset):
            begin = (level + group[1]) % levels * width + offset
            where = pl.ds(pl.multiple_of(begin, SUB), SUB)
            return jnp.concatenate([ref[:, where, :] for ref in group[0]], axis=0)

        def outside(ref):
            return ref[:, pl.ds(pl.multiple_of(level * SUB, SUB), SUB), :]

        right = block(second, 0) if inside else outside(after)
        left = block(first, width - SUB) if inside else outside(before)
        both = [
            (
                block(first, PSIDE),
                block(first, PSIDE + SUB),
                jnp.where(near, right, block(first, PSIDE - SUB)),
            ),
            (block(second, 0), block(second, SUB), jnp.where(near, block(second, PSIDE), left)),
        ]
        for p, pieces in enumerate(both):
            table = jnp.dot(
                expand, tables[p, level], precision=HIGHEST, preferred_element_type=jnp.float32
            )
            spread, scaled, pull = [], [], 0.0
            for g, piece in enumerate(pieces):
                x = piece.reshape(cells, members)
                mean = jnp.mean(x, axis=1, keepdims=True)
                y = x - mean
                w = jnp.sum(jnp.where(lane == g * SUB + sub, table, 0.0), axis=1, keepdims=True)
                u = jnp.sum(
                    jnp.where(lane == SPAN + g * SUB + sub, table, 0.0), axis=1, keepdims=True
                )
                pull = pull + jnp.sum(y * (u - w * mean), axis=0, keepdims=True)
                spread.append(y)
                scaled.append(y * w)
            y = split(jnp.concatenate(spread, axis=0))
            z = split(jnp.concatenate(scaled, axis=0))
            gram[p] += dot3(z, y, ((0,), (0,)))
            pulled[p] += pull
        return carry

    lax.fori_loop(0, levels, step, 0)
    results = roots_of([gram[0], gram[1]], [pulled[0], pulled[1]], ITERS)
    for p, (group, offset) in enumerate(((first, PSIDE), (second, 0))):
        root, mean_weight = results[p]
        for level in range(levels):
            begin = (level + group[1]) % levels * width + offset
            x = group[0][1][:, begin : begin + PSIDE, :]
            x = x.reshape(rows * PSIDE, members)
            centre = jnp.mean(x, axis=1, keepdims=True)
            d = x - centre
            moved = centre + jnp.sum(d * mean_weight, axis=1, keepdims=True)
            mixed = moved + dot3(split(d), root)
            begin = (level + turn) % levels * width + p * PSIDE
            out[:, begin : begin + PSIDE, :] = mixed.reshape(rows, PSIDE, members)


def estimate(flops, *arrays):
    moved = sum(a.size * a.dtype.itemsize for a in arrays)
    return pl.CostEstimate(flops=flops, bytes_accessed=moved, transcendentals=0)


def pack(background, nx, ny, turn, width):
    here, levels, lat_rows, lon_cells = background.shape
    lat = lat_rows // ny
    shape = jax.ShapeDtypeStruct((nx, ny, here, lat, levels * width), background.dtype)
    return pl.pallas_call(
        functools.partial(pack_kernel, ny, turn, width),
        out_shape=shape,
        grid=(here,),
        in_specs=[pl.BlockSpec((1, levels, lat_rows, lon_cells), lambda h: (h, 0, 0, 0))],
        out_specs=pl.BlockSpec((nx, ny, 1, lat, levels * width), lambda h: (0, 0, h, 0, 0)),
        cost_estimate=estimate(0, background, shape),
        compiler_params=pltpu.CompilerParams(vmem_limit_bytes=SMALL_LIMIT),
    )(background)


def unpack(chunks, shape):
    nx, ny, here, lat, lanes = chunks[0].shape
    return pl.pallas_call(
        unpack_kernel,
        out_shape=jax.ShapeDtypeStruct(shape, chunks[0].dtype),
        grid=(here,),
        in_specs=[pl.BlockSpec((nx, ny, 1, lat, lanes), lambda h: (0, 0, h, 0, 0))] * len(chunks),
        out_specs=pl.BlockSpec((1, *shape[1:]), lambda h: (h, 0, 0, 0)),
        cost_estimate=estimate(0, *chunks, *chunks),
        compiler_params=pltpu.CompilerParams(vmem_limit_bytes=SMALL_LIMIT),
    )(*chunks)


def analyse(turn, inside, inputs, levels):
    core = inputs[1]
    members = core.shape[2]
    shape = jax.ShapeDtypeStruct(core.shape, core.dtype)
    vmem = pl.BlockSpec(memory_space=pltpu.VMEM)
    flops = 6 * 2 * members**2 * (levels * SPAN * SPAN + levels * PSIDE * PSIDE + 12 * members)
    return pl.pallas_call(
        functools.partial(pair_kernel, turn, inside),
        out_shape=shape,
        in_specs=[vmem] * (len(inputs) - 1) + [pl.BlockSpec(memory_space=pltpu.HBM)],
        out_specs=vmem,
        scratch_shapes=[
            pltpu.VMEM((2, members, members), jnp.float32),
            pltpu.VMEM((2, 1, members), jnp.float32),
        ],
        cost_estimate=estimate(5 * flops, *inputs[:-1], shape),
        compiler_params=pltpu.CompilerParams(vmem_limit_bytes=VMEM_LIMIT),
    )(*inputs)


def tables_of(obs_cells, obs_counts, obs_widths, obs_values, obs_variances, levels):
    level_of = obs_cells // (SPAN * SPAN)
    row = obs_cells // SPAN % SPAN
    col = obs_cells % SPAN
    row_out = jnp.maximum(jnp.maximum(HALO - row, row - (HALO + PSIDE - 1)), 0)
    col_out = jnp.maximum(jnp.maximum(HALO - col, col - (HALO + PSIDE - 1)), 0)
    distance = jnp.maximum(row_out, col_out)
    slots = lax.broadcasted_iota(jnp.int32, obs_cells.shape, 1)
    usable = (slots < obs_counts[:, None]) & (distance <= obs_widths[:, None])
    relative = distance.astype(jnp.float32) / (obs_widths[:, None] + 1).astype(jnp.float32)
    weights = jnp.where(usable, jnp.exp(-relative * relative) / obs_variances, 0.0)
    place = jnp.where(
        col < HALO,
        PSIDE + HALO + col,
        col - HALO,
    )
    line = level_of * SPAN + row
    hot_line = (line[:, :, None] == jnp.arange(levels * SPAN)).astype(jnp.float32)
    hot_place = place[:, :, None] == jnp.arange(SPAN)
    sums = jnp.concatenate(
        [
            jnp.where(hot_place, weights[:, :, None], 0.0),
            jnp.where(hot_place, (weights * obs_values)[:, :, None], 0.0),
        ],
        axis=2,
    )
    table = jnp.einsum("psl,psg->plg", hot_line, sums, precision=HIGHEST)
    return table.reshape(table.shape[0], levels, SPAN, 2 * SPAN)


def shift(x, axis, step, wrap):
    n = lax.axis_size(axis)
    pairs = [(i, (i + step) % n) for i in range(n) if wrap or 0 <= i + step < n]
    return lax.ppermute(x, axis, pairs)


def shards(background, obs_cells, obs_counts, obs_widths, obs_values, obs_variances):
    here, levels, lat_rows, lon_cells = background.shape
    nx = lax.axis_size("gx")
    ny = lax.axis_size("gy")
    lat = lat_rows // ny
    lon = lon_cells // nx
    members = nx * ny * here
    width = 2 * PSIDE
    number = lon // width
    tables = tables_of(
        obs_cells[0], obs_counts[0], obs_widths[0], obs_values[0], obs_variances[0], levels
    )

    def exchange(x):
        return lax.all_to_all(x, ("gx", "gy"), split_axis=0, concat_axis=0, tiled=True)

    def section(group, turn, begin):
        def pick(x):
            x = x.reshape(x.shape[0], levels, width, members)[:, :, begin : begin + SUB]
            x = jnp.roll(x, -turn, axis=1)
            return x.reshape(x.shape[0], levels * SUB, members)

        return jnp.concatenate([pick(x) for x in group], axis=0)

    def halo_of(core):
        up = shift(core[lat - HALO :], "gy", 1, False)
        return up, shift(core[:HALO], "gy", -1, False)

    def with_core(q):
        return halos[q][0], cores[q], halos[q][1]

    last = number - 1
    transfers, cores, halos = [], [], []
    for q in range(number):
        send = pack(background, nx, ny, q, width).reshape(members, lat, levels * width)
        if q >= 2:
            send, halos[q - 2] = lax.optimization_barrier((send, halos[q - 2]))
        transfers.append(exchange(send))
        cores.append(jnp.transpose(transfers[q], (1, 2, 0)))
        halos.append(halo_of(cores[q]))
    after = shift(section(with_core(0), 0, 0), "gx", -1, True)
    before = None
    for c in range(number):
        table = tables[2 * c + 1 : 2 * c + 3] if c < last else jnp.stack([tables[-1], tables[0]])
        inputs = (*with_core(c), *with_core((c + 1) % number))
        if c == last:
            inputs = (*inputs, after, before)
        mixed = analyse(c, c < last, (*inputs, table, transfers[c + 2]), levels)
        back = jnp.transpose(mixed, (2, 0, 1))
        if c == 0:
            back, halos[last - 1] = lax.optimization_barrier((back, halos[last - 1]))
        if c == 1:
            back, halos[last], after = lax.optimization_barrier((back, halos[last], after))
            before = shift(section(with_core(last), last, width - SUB), "gx", 1, True)
        if c == 2:
            back, before = lax.optimization_barrier((back, before))
        if c == 0:
            back, transfers[last] = lax.optimization_barrier((back, transfers[last]))
        transfers.append(exchange(back))
    chunks = [t.reshape(nx, ny, here, lat, levels * width) for t in transfers[number:]]
    return unpack(chunks, background.shape)


def solution(mesh):
    return jax.shard_map(
        shards,
        mesh=mesh,
        in_specs=(
            P(("gx", "gy"), None, None, None),
            P("gy", "gx", None),
            P("gy", "gx"),
            P("gy", "gx"),
            P("gy", "gx", None),
            P("gy", "gx", None),
        ),
        out_specs=P(("gx", "gy"), None, None, None),
        check_vma=False,
    )
```

```python
import functools

import jax
import jax.numpy as jnp
from jax import lax
from jax.experimental import pallas as pl
from jax.experimental.pallas import tpu as pltpu
from jax.sharding import PartitionSpec as P

PSIDE = 16
HALO = 4
ITERS = 5
SUB = 8
SPAN = PSIDE + 2 * HALO
HIGHEST = lax.Precision.HIGHEST
VMEM_LIMIT = 32 * 1024 * 1024
SMALL_LIMIT = 60 * 1024 * 1024


def split(x):
    high = x.astype(jnp.bfloat16)
    return high, (x - high.astype(jnp.float32)).astype(jnp.bfloat16)


def dot3(a, b, dims=((1,), (0,))):
    def one(x, y):
        return lax.dot_general(x, y, (dims, ((), ())), preferred_element_type=jnp.float32)

    return one(a[0], b[0]) + (one(a[0], b[1]) + one(a[1], b[0]))


def pack_kernel(ny, turn, width, source, out):
    levels = source.shape[1]
    lat = source.shape[2] // ny
    lon = source.shape[3] // out.shape[0]
    shape = (source.shape[2], lon)
    group = lax.broadcasted_iota(jnp.int32, shape, 1) // width
    for x in range(out.shape[0]):
        whole = source[0, 0, :, x * lon : (x + 1) * lon]
        for level in range(1, levels):
            part = source[0, level, :, x * lon : (x + 1) * lon]
            part = pltpu.roll(part, level * width, 1)
            whole = jnp.where(group == (turn + level) % levels, part, whole)
        out[x, :, 0] = whole.reshape(ny, lat, lon)


def unpack_kernel(*refs):
    *chunks, out = refs
    levels = out.shape[1]
    ny, lat, lon = chunks[0].shape[1], chunks[0].shape[3], chunks[0].shape[4]
    width = lon // levels
    group = lax.broadcasted_iota(jnp.int32, (ny * lat, lon), 1) // width
    for x in range(chunks[0].shape[0]):
        parts = [chunk[x, :, 0].reshape(ny * lat, lon) for chunk in chunks]
        for level in range(levels):
            whole = parts[0]
            for turn in range(1, len(parts)):
                whole = jnp.where(group == (turn + level) % levels, parts[turn], whole)
            back = (PSIDE - level * width) % lon
            out[0, level, :, x * lon : (x + 1) * lon] = pltpu.roll(whole, back, 1)


def roots_of(grams, pulls, sweeps):
    members = grams[0].shape[0]
    eye = (
        lax.broadcasted_iota(jnp.int32, (members, members), 0)
        == lax.broadcasted_iota(jnp.int32, (members, members), 1)
    ).astype(jnp.float32)
    divisors, currents = [], []
    for g in grams:
        square = jnp.sum(jnp.sum(g * g, axis=0, keepdims=True), axis=1, keepdims=True)
        divisor = members - 1.0 + jnp.sqrt(square)
        divisors.append(divisor)
        currents.append((g + (members - 1.0) * eye) / divisor)
    roots = None
    for repeat in range(sweeps):
        cur = [split(c) for c in currents]
        if repeat == 0:
            factors = [1.5 * eye - 0.5 * c for c in currents]
            fac = [split(f) for f in factors]
            roots = factors
        else:
            old = [split(r) for r in roots]
            factors = [1.5 * eye - 0.5 * dot3(r, c) for r, c in zip(old, cur)]
            fac = [split(f) for f in factors]
            roots = [dot3(f, r) for f, r in zip(fac, old)]
        if repeat < sweeps - 1:
            currents = [dot3(c, f) for c, f in zip(cur, fac)]
    results = []
    for divisor, root, pull in zip(divisors, roots, pulls):
        half = jnp.sum(root * pull, axis=1, keepdims=True)
        mean = jnp.sum(root * half, axis=0, keepdims=True) / divisor
        results.append((split(jnp.sqrt((members - 1.0) / divisor) * root), mean))
    return results


def pair_kernel(turn, inside, *refs):
    first, second, refs = (refs[:3], turn), (refs[3:6], turn + 1), refs[6:]
    if inside:
        tables, _, out, gram, pulled = refs
    else:
        after, before, tables, _, out, gram, pulled = refs
    rows, lanes, members = first[0][1].shape
    levels = tables.shape[1]
    width = lanes // levels
    cells = SPAN * SUB
    cell_row = lax.broadcasted_iota(jnp.int32, (cells, SPAN), 0) // SUB
    expand = (cell_row == lax.broadcasted_iota(jnp.int32, (cells, SPAN), 1)).astype(jnp.float32)
    sub = lax.broadcasted_iota(jnp.int32, (cells, 2 * SPAN), 0) % SUB
    lane = lax.broadcasted_iota(jnp.int32, (cells, 2 * SPAN), 1)
    near = lax.broadcasted_iota(jnp.int32, (SPAN, SUB, members), 1) < HALO
    gram[...] = jnp.zeros_like(gram)
    pulled[...] = jnp.zeros_like(pulled)

    def step(level, carry):
        def block(group, offset):
            begin = (level + group[1]) % levels * width + offset
            where = pl.ds(pl.multiple_of(begin, SUB), SUB)
            return jnp.concatenate([ref[:, where, :] for ref in group[0]], axis=0)

        def outside(ref):
            return ref[:, pl.ds(pl.multiple_of(level * SUB, SUB), SUB), :]

        right = block(second, 0) if inside else outside(after)
        left = block(first, width - SUB) if inside else outside(before)
        both = [
            (
                block(first, PSIDE),
                block(first, PSIDE + SUB),
                jnp.where(near, right, block(first, PSIDE - SUB)),
            ),
            (block(second, 0), block(second, SUB), jnp.where(near, block(second, PSIDE), left)),
        ]
        for p, pieces in enumerate(both):
            table = jnp.dot(
                expand, tables[p, level], precision=HIGHEST, preferred_element_type=jnp.float32
            )
            spread, scaled, pull = [], [], 0.0
            for g, piece in enumerate(pieces):
                x = piece.reshape(cells, members)
                mean = jnp.mean(x, axis=1, keepdims=True)
                y = x - mean
                w = jnp.sum(jnp.where(lane == g * SUB + sub, table, 0.0), axis=1, keepdims=True)
                u = jnp.sum(
                    jnp.where(lane == SPAN + g * SUB + sub, table, 0.0), axis=1, keepdims=True
                )
                pull = pull + jnp.sum(y * (u - w * mean), axis=0, keepdims=True)
                spread.append(y)
                scaled.append(y * w)
            y = split(jnp.concatenate(spread, axis=0))
            z = split(jnp.concatenate(scaled, axis=0))
            gram[p] += dot3(z, y, ((0,), (0,)))
            pulled[p] += pull
        return carry

    lax.fori_loop(0, levels, step, 0)
    results = roots_of([gram[0], gram[1]], [pulled[0], pulled[1]], ITERS)
    for p, (group, offset) in enumerate(((first, PSIDE), (second, 0))):
        root, mean_weight = results[p]
        for level in range(levels):
            begin = (level + group[1]) % levels * width + offset
            x = group[0][1][:, begin : begin + PSIDE, :]
            x = x.reshape(rows * PSIDE, members)
            centre = jnp.mean(x, axis=1, keepdims=True)
            d = x - centre
            moved = centre + jnp.sum(d * mean_weight, axis=1, keepdims=True)
            mixed = moved + dot3(split(d), root)
            begin = (level + turn) % levels * width + p * PSIDE
            out[:, begin : begin + PSIDE, :] = mixed.reshape(rows, PSIDE, members)


def estimate(flops, *arrays):
    moved = sum(a.size * a.dtype.itemsize for a in arrays)
    return pl.CostEstimate(flops=flops, bytes_accessed=moved, transcendentals=0)


def pack(background, nx, ny, turn, width):
    here, levels, lat_rows, lon_cells = background.shape
    lat = lat_rows // ny
    shape = jax.ShapeDtypeStruct((nx, ny, here, lat, levels * width), background.dtype)
    return pl.pallas_call(
        functools.partial(pack_kernel, ny, turn, width),
        out_shape=shape,
        grid=(here,),
        in_specs=[pl.BlockSpec((1, levels, lat_rows, lon_cells), lambda h: (h, 0, 0, 0))],
        out_specs=pl.BlockSpec((nx, ny, 1, lat, levels * width), lambda h: (0, 0, h, 0, 0)),
        cost_estimate=estimate(0, background, shape),
        compiler_params=pltpu.CompilerParams(vmem_limit_bytes=SMALL_LIMIT),
    )(background)


def unpack(chunks, shape):
    nx, ny, here, lat, lanes = chunks[0].shape
    return pl.pallas_call(
        unpack_kernel,
        out_shape=jax.ShapeDtypeStruct(shape, chunks[0].dtype),
        grid=(here,),
        in_specs=[pl.BlockSpec((nx, ny, 1, lat, lanes), lambda h: (0, 0, h, 0, 0))] * len(chunks),
        out_specs=pl.BlockSpec((1, *shape[1:]), lambda h: (h, 0, 0, 0)),
        cost_estimate=estimate(0, *chunks, *chunks),
        compiler_params=pltpu.CompilerParams(vmem_limit_bytes=SMALL_LIMIT),
    )(*chunks)


def analyse(turn, inside, inputs, levels):
    core = inputs[1]
    members = core.shape[2]
    shape = jax.ShapeDtypeStruct(core.shape, core.dtype)
    vmem = pl.BlockSpec(memory_space=pltpu.VMEM)
    flops = 6 * 2 * members**2 * (levels * SPAN * SPAN + levels * PSIDE * PSIDE + 12 * members)
    return pl.pallas_call(
        functools.partial(pair_kernel, turn, inside),
        out_shape=shape,
        in_specs=[vmem] * (len(inputs) - 1) + [pl.BlockSpec(memory_space=pltpu.HBM)],
        out_specs=vmem,
        scratch_shapes=[
            pltpu.VMEM((2, members, members), jnp.float32),
            pltpu.VMEM((2, 1, members), jnp.float32),
        ],
        cost_estimate=estimate(5 * flops, *inputs[:-1], shape),
        compiler_params=pltpu.CompilerParams(vmem_limit_bytes=VMEM_LIMIT),
    )(*inputs)


def tables_of(obs_cells, obs_counts, obs_widths, obs_values, obs_variances, levels):
    level_of = obs_cells // (SPAN * SPAN)
    row = obs_cells // SPAN % SPAN
    col = obs_cells % SPAN
    row_out = jnp.maximum(jnp.maximum(HALO - row, row - (HALO + PSIDE - 1)), 0)
    col_out = jnp.maximum(jnp.maximum(HALO - col, col - (HALO + PSIDE - 1)), 0)
    distance = jnp.maximum(row_out, col_out)
    slots = lax.broadcasted_iota(jnp.int32, obs_cells.shape, 1)
    usable = (slots < obs_counts[:, None]) & (distance <= obs_widths[:, None])
    relative = distance.astype(jnp.float32) / (obs_widths[:, None] + 1).astype(jnp.float32)
    weights = jnp.where(usable, jnp.exp(-relative * relative) / obs_variances, 0.0)
    place = jnp.where(
        col < HALO,
        PSIDE + HALO + col,
        col - HALO,
    )
    line = level_of * SPAN + row
    hot_line = (line[:, :, None] == jnp.arange(levels * SPAN)).astype(jnp.float32)
    hot_place = place[:, :, None] == jnp.arange(SPAN)
    sums = jnp.concatenate(
        [
            jnp.where(hot_place, weights[:, :, None], 0.0),
            jnp.where(hot_place, (weights * obs_values)[:, :, None], 0.0),
        ],
        axis=2,
    )
    table = jnp.einsum("psl,psg->plg", hot_line, sums, precision=HIGHEST)
    return table.reshape(table.shape[0], levels, SPAN, 2 * SPAN)


def shift(x, axis, step, wrap):
    n = lax.axis_size(axis)
    pairs = [(i, (i + step) % n) for i in range(n) if wrap or 0 <= i + step < n]
    return lax.ppermute(x, axis, pairs)


def shards(background, obs_cells, obs_counts, obs_widths, obs_values, obs_variances):
    here, levels, lat_rows, lon_cells = background.shape
    nx = lax.axis_size("gx")
    ny = lax.axis_size("gy")
    lat = lat_rows // ny
    lon = lon_cells // nx
    members = nx * ny * here
    width = 2 * PSIDE
    number = lon // width
    tables = tables_of(
        obs_cells[0], obs_counts[0], obs_widths[0], obs_values[0], obs_variances[0], levels
    )

    def exchange(x):
        return lax.all_to_all(x, ("gx", "gy"), split_axis=0, concat_axis=0, tiled=True)

    def section(group, turn, begin):
        def pick(x):
            x = x.reshape(x.shape[0], levels, width, members)[:, :, begin : begin + HALO]
            x = jnp.roll(x, -turn, axis=1)
            return x.reshape(x.shape[0], levels * HALO, members)

        return jnp.concatenate([pick(x) for x in group], axis=0)

    def widen(x, low):
        x = x.reshape(x.shape[0], levels, HALO, members)
        x = jnp.pad(x, ((0, 0), (0, 0), (low, SUB - HALO - low), (0, 0)))
        return x.reshape(x.shape[0], levels * SUB, members)

    def halo_of(core):
        up = shift(core[lat - HALO :], "gy", 1, False)
        return up, shift(core[:HALO], "gy", -1, False)

    def with_core(q):
        return halos[q][0], cores[q], halos[q][1]

    last = number - 1
    transfers, cores, halos = [], [], []
    for q in range(number):
        send = pack(background, nx, ny, q, width).reshape(members, lat, levels * width)
        if q >= 2:
            send, halos[q - 2] = lax.optimization_barrier((send, halos[q - 2]))
        transfers.append(exchange(send))
        cores.append(jnp.transpose(transfers[q], (1, 2, 0)))
        halos.append(halo_of(cores[q]))
    after = shift(section(with_core(0), 0, 0), "gx", -1, True)
    before = None
    for c in range(number):
        table = tables[2 * c + 1 : 2 * c + 3] if c < last else jnp.stack([tables[-1], tables[0]])
        inputs = (*with_core(c), *with_core((c + 1) % number))
        if c == last:
            inputs = (*inputs, widen(after, 0), widen(before, SUB - HALO))
        mixed = analyse(c, c < last, (*inputs, table, transfers[c + 2]), levels)
        back = jnp.transpose(mixed, (2, 0, 1))
        if c == 0:
            back, halos[last - 1] = lax.optimization_barrier((back, halos[last - 1]))
        if c == 1:
            back, halos[last], after = lax.optimization_barrier((back, halos[last], after))
            before = shift(section(with_core(last), last, width - HALO), "gx", 1, True)
        if c == 2:
            back, before = lax.optimization_barrier((back, before))
        if c == 0:
            back, transfers[last] = lax.optimization_barrier((back, transfers[last]))
        transfers.append(exchange(back))
    chunks = [t.reshape(nx, ny, here, lat, levels * width) for t in transfers[number:]]
    return unpack(chunks, background.shape)


def solution(mesh):
    return jax.shard_map(
        shards,
        mesh=mesh,
        in_specs=(
            P(("gx", "gy"), None, None, None),
            P("gy", "gx", None),
            P("gy", "gx"),
            P("gy", "gx"),
            P("gy", "gx", None),
            P("gy", "gx", None),
        ),
        out_specs=P(("gx", "gy"), None, None, None),
        check_vma=False,
    )
```
